32 devices in a mesh: models: 1, leaf: 32 (over z, y, x, core).
Axes of the slice: x: 2, y: 2, z: 4, core: 2. Of those that a mesh axis runs over, the one named last changes fastest.
Arguments:
- slip_rate: float32 [131072], P(('models', 'leaf')), may hold values from -6 to 6
- near_blocks: bfloat16 [512, 3, 256, 256], P(('models', 'leaf')), may hold values from -0.21875 to 0.21875
- near_index: int32 [512, 3], P(('models', 'leaf')), may hold values from 0 to 511, as said below
- far_left: bfloat16 [9, 32, 131072], P(None, None, ('models', 'leaf')), may hold values from -1 to 1
- far_right: bfloat16 [9, 32, 131072], P(None, None, ('models', 'leaf')), may hold values from -6 to 6
- far_ranks: int32 [512, 9], P(('models', 'leaf')), may hold values from 8 to 32
Outputs:
- first_stress: float32 [131072], P(('models', 'leaf'))
- second_stress: float32 [131072], P(('models', 'leaf'))
The draws below stay inside these ranges and needn't reach their ends.
Inputs may be any that keep to these rules, and one draw needn't show every extreme that they name: near_index[i, 0] = i; every other entry is a leaf j != i with |j - i| <= 16, and distance 16 occurs.
All inputs are finite; a program needn't handle non-finite values.
Results may differ from the reference program's by a relative error of at most 0.0045.
Values may be sent and summed in bfloat16 or wider, within the bound.
A program may use at most 64 MiB of HBM per device.

```python
import math
import jax
import jax.numpy as jnp
from jax import lax

LEAF = 256
RANK = 32
NEAR = 3
LEAVES_DEV = 16
LEAVES = 512
PATCHES = 131072
LEVELS = 9


def draw_near_index(key, part):
    base_key = jax.random.fold_in(key, 11)
    key_size, key_sign = jax.random.split(base_key)
    distance = jax.random.randint(key_size, (LEAVES, NEAR - 1), 1, LEAVES_DEV + 1)
    direction = jax.random.randint(key_sign, (LEAVES, NEAR - 1), 0, 2) * 2 - 1
    anchor = jnp.arange(LEAVES, dtype=jnp.int32)[:, None]
    target = anchor + direction * distance
    target = jnp.where((target < 0) | (target >= LEAVES), anchor - direction * distance, target)
    return jnp.concatenate([anchor, target], axis=1).astype(jnp.int32)


def set_ends(array, rng, smallest, high):
    longest = array.shape.index(max(array.shape))
    spots = []
    for shift in (0, 1):
        where = [jax.random.randint(jax.random.fold_in(rng, axis), (), 0, length) for axis, length in enumerate(array.shape)]
        where[longest] = (where[longest] + shift) % array.shape[longest]
        spots.append(tuple(where))
    return array.at[spots[0]].set(smallest).at[spots[1]].set(high)


def block_scale(rng, extent, cuts, low, high):
    def one(position, shards_of):
        steps = jax.random.uniform(jax.random.fold_in(jax.random.fold_in(rng, 6), position), (shards_of,), jnp.float32, low / len(cuts), high / len(cuts))
        return jnp.repeat(jnp.exp(steps), extent[position] // shards_of).reshape((-1,) + (1,) * (len(extent) - position - 1))

    level = one(*cuts[0])
    for cut in cuts[1:]:
        level = level * one(*cut)
    return level


def scatter_about(stream_key, dims, spread, limit, shards=(), kind=jnp.bfloat16):
    values = jax.random.normal(stream_key, dims, jnp.float32) * spread
    if len(shards) > 0:
        values = block_scale(stream_key, dims, shards, -0.22, 0.18) * values
    return jnp.clip(values, min=-limit, max=limit).astype(kind)


def setup_inputs(seed: int = 0, part: int = 0) -> dict:
    splits = jax.random.split(jax.random.key(seed), 7)
    own_keys = jax.random.split(jax.random.fold_in(splits[6], part), 7)
    return {
        "slip_rate": scatter_about(own_keys[0], (PATCHES,), 1.0, 6.0, ((0, 32),), jnp.float32),
        "near_blocks": scatter_about(own_keys[1], (LEAVES, NEAR, LEAF, LEAF), (NEAR * LEAF) ** -0.5, 0.21875, ((0, 32),)),
        "near_index": draw_near_index(jax.random.fold_in(jax.random.fold_in(splits[6], part), 71), part),
        "far_left": scatter_about(own_keys[3], (LEVELS, RANK, PATCHES), RANK ** -0.5, 1.0, ((2, 32),)),
        "far_right": scatter_about(own_keys[4], (LEVELS, RANK, PATCHES), 1.0, 6.0, ((2, 32),)),
        "far_ranks": set_ends(jax.random.randint(own_keys[5], (LEAVES, LEVELS), RANK // 4, RANK + 1), jax.random.fold_in(own_keys[5], 1), RANK // 4, RANK).astype(jnp.int32),
    }


def matvec(operand, near_blocks, near_index, far_left, far_right, far_ranks):
    leaves = near_blocks.shape[0]
    leaf_size = near_blocks.shape[2]
    levels = far_left.shape[0]
    rank_cols = far_left.shape[1]
    slip_rows = operand.reshape(leaves, leaf_size)
    picked = slip_rows[near_index].astype(jnp.float32)
    result = jnp.einsum('ikpq,ikq->ip', near_blocks.astype(jnp.float32), picked)
    rank_iota = jnp.arange(rank_cols, dtype=jnp.int32)
    rows_float = slip_rows.astype(jnp.float32)
    for level_no in range(levels):
        span_size = 2 ** level_no
        right_part = far_right[level_no].reshape(rank_cols, leaves, leaf_size).astype(jnp.float32)
        projected = jnp.einsum('rcp,cp->cr', right_part, rows_float)
        cluster_sums = projected.reshape(leaves // span_size, span_size, rank_cols).sum(axis=1)
        cluster_sums = cluster_sums * (1.0 / math.sqrt(leaf_size * span_size))
        partner = cluster_sums.reshape(-1, 2, rank_cols)[:, ::-1, :].reshape(-1, rank_cols)
        partner = jnp.repeat(partner, span_size, axis=0)
        masked = jnp.where(rank_iota[None, :] < far_ranks[:, level_no:level_no + 1], partner, 0.0)
        weights = lax.optimization_barrier(masked.astype(jnp.bfloat16))
        left_part = far_left[level_no].reshape(rank_cols, leaves, leaf_size).astype(jnp.float32)
        result = result + jnp.einsum('rcp,cr->cp', left_part, weights.astype(jnp.float32))
    return result.reshape(-1)

def reference(slip_rate, near_blocks, near_index, far_left, far_right, far_ranks):
    slip_bf = lax.optimization_barrier(slip_rate.astype(jnp.bfloat16))
    first_stress = matvec(slip_bf, near_blocks, near_index, far_left, far_right, far_ranks)
    relaxed = slip_rate + jnp.tanh(first_stress / 3.0)
    relaxed_bf = lax.optimization_barrier(relaxed.astype(jnp.bfloat16))
    second_stress = matvec(relaxed_bf, near_blocks, near_index, far_left, far_right, far_ranks)
    return (first_stress, second_stress)
```

```python
import functools
import math

import jax
import jax.numpy as jnp
from jax import lax
from jax.experimental import pallas as pl
from jax.experimental.pallas import tpu as pltpu
from jax.sharding import PartitionSpec as P

MESH = pl.DeviceIdType.MESH
LANES = 128
F32 = jnp.float32
BF16 = jnp.bfloat16


def flipped(me, slot):
    target = me
    bit = 1
    while bit <= slot:
        if slot & bit:
            target = target + bit * (1 - 2 * ((me // bit) % 2))
        bit *= 2
    return target


def dot_nt(a, b):
    return lax.dot_general(a, b, (((1,), (1,)), ((), ())), preferred_element_type=F32)


def dot_nn(a, b):
    return lax.dot_general(a, b, (((1,), (0,)), ((), ())), preferred_element_type=F32)


def kernel(
    n, levels, ranks_n,
    slip_ref, near_hbm, index_ref, left_hbm, right_hbm, ranks_ref,
    first_ref, second_ref,
    near_v, left_v, right_v, ext_first, ext_second, pick, dev, recv, scale_ref,
    near_sem, left_sem, right_sem, halo_send, halo_recv, far_send, far_recv,
):
    me = lax.axis_index("leaf")
    ext = (ext_first, ext_second)
    leaves, near_n, size, _ = near_v.shape
    local_levels = leaves.bit_length() - 1
    cross = levels - local_levels
    cols = levels * ranks_n
    local_cols = local_levels * ranks_n
    per_chunk = LANES // ranks_n
    right_parts = right_sem.shape[0]
    near_parts = near_sem.shape[0]
    right_width = right_v.shape[1] // right_parts
    near_width = leaves // near_parts

    barrier = pltpu.get_barrier_semaphore()
    for slot in range(1, n):
        pl.semaphore_signal(
            barrier, inc=1, device_id={"leaf": flipped(me, slot)}, device_id_type=MESH
        )

    right_copies = [
        pltpu.make_async_copy(
            right_hbm.at[:, pl.ds(part * right_width, right_width)],
            right_v.at[:, pl.ds(part * right_width, right_width)],
            right_sem.at[part],
        )
        for part in range(right_parts)
    ]
    near_copies = [
        pltpu.make_async_copy(
            near_hbm.at[pl.ds(part * near_width, near_width)],
            near_v.at[pl.ds(part * near_width, near_width)],
            near_sem.at[part],
        )
        for part in range(near_parts)
    ]
    left_copy = pltpu.make_async_copy(left_hbm, left_v, left_sem)
    for copy in right_copies:
        copy.start()
    for copy in near_copies[:1]:
        copy.start()
    left_copy.start()
    for copy in near_copies[1:]:
        copy.start()

    slip = jnp.concatenate(
        [slip_ref[pl.ds(half, leaves, stride=2), :] for half in range(2)], axis=1
    )
    dev[...] = jnp.zeros_like(dev)

    col = lax.broadcasted_iota(jnp.int32, (leaves, cols), 1)
    allowed = jnp.zeros((leaves, cols), jnp.int32)
    scale = jnp.zeros((leaves, cols), F32)
    ranks = ranks_ref[...]
    for level in range(levels):
        here = (col >= level * ranks_n) & (col < (level + 1) * ranks_n)
        allowed = jnp.where(here, ranks[:, level : level + 1] + level * ranks_n, allowed)
        scale = jnp.where(here, 1.0 / math.sqrt(size * 2**level), scale)
    scale_ref[...] = jnp.where(col < allowed, scale, 0.0)

    row_cols = lax.broadcasted_iota(jnp.int32, (leaves, cols), 0)
    row_size = lax.broadcasted_iota(jnp.int32, (leaves, size), 0)
    row_lane = lax.broadcasted_iota(jnp.int32, (leaves, LANES), 0)
    lane = lax.broadcasted_iota(jnp.int32, (leaves, LANES), 1)

    def halo_copies(call):
        own = ext[call].at[pl.ds(leaves, leaves)]
        up = pltpu.make_async_remote_copy(
            src_ref=own, dst_ref=ext[call].at[pl.ds(0, leaves)],
            send_sem=halo_send.at[call, 0], recv_sem=halo_recv.at[call, 0],
            device_id={"leaf": me + 1}, device_id_type=MESH,
        )
        down = pltpu.make_async_remote_copy(
            src_ref=own, dst_ref=ext[call].at[pl.ds(2 * leaves, leaves)],
            send_sem=halo_send.at[call, 1], recv_sem=halo_recv.at[call, 1],
            device_id={"leaf": me - 1}, device_id_type=MESH,
        )
        return up, down

    def send_halo(call):
        up, down = halo_copies(call)

        @pl.when(me < n - 1)
        def _():
            up.start()

        @pl.when(me > 0)
        def _():
            down.start()

    def receive_halo(call):
        up, down = halo_copies(call)

        @pl.when(me < n - 1)
        def _():
            up.wait_send()
            down.wait_recv()

        @pl.when(me > 0)
        def _():
            down.wait_send()
            up.wait_recv()

    def project(vector, call):
        projected = jnp.zeros((leaves, cols), F32)
        for c in range(leaves):
            if call == 0 and (c * size) % right_width == 0:
                right_copies[c * size // right_width].wait()
            part = dot_nt(vector, right_v[:, c * size : (c + 1) * size])
            projected = jnp.where(row_cols == c, part, projected)
        total = jnp.sum(projected[:, local_cols:], axis=0, keepdims=True)
        chunks = dev.shape[1]
        for chunk in range(chunks):
            width = min(LANES, total.shape[1] - chunk * LANES)
            dev[call, chunk : chunk + 1, 0:width] = total[:, chunk * LANES : chunk * LANES + width]
        return projected[:, :local_cols]

    def send_far(call):
        for slot in range(n - 1, 0, -1):
            chunk = (slot.bit_length() - 1) // per_chunk
            pltpu.make_async_remote_copy(
                src_ref=dev.at[call, pl.ds(chunk, 1)],
                dst_ref=recv.at[call, pl.ds(slot, 1)],
                send_sem=far_send.at[call], recv_sem=far_recv.at[call],
                device_id={"leaf": flipped(me, slot)}, device_id_type=MESH,
            ).start()

    def receive_far(call):
        rows = recv.at[call, pl.ds(1, n - 1)]
        pltpu.make_async_copy(rows, rows, far_send.at[call]).wait()
        pltpu.make_async_copy(rows, rows, far_recv.at[call]).wait()
        got = recv[call]
        slot = lax.broadcasted_iota(jnp.int32, (n, LANES), 0)
        slot_lane = lax.broadcasted_iota(jnp.int32, (n, LANES), 1)
        pieces = []
        for chunk in range(dev.shape[1]):
            keep = slot < 0
            for bit in range(chunk * per_chunk, min(cross, (chunk + 1) * per_chunk)):
                low = (bit - chunk * per_chunk) * ranks_n
                keep = keep | (
                    (slot >= 2**bit) & (slot < 2 ** (bit + 1))
                    & (slot_lane >= low) & (slot_lane < low + ranks_n)
                )
            piece = jnp.sum(jnp.where(keep, got, 0.0), axis=0, keepdims=True)
            width = min(LANES, cross * ranks_n - chunk * LANES)
            pieces.append(jnp.broadcast_to(piece, (leaves, LANES))[:, :width])
        sums = pieces[0] if len(pieces) == 1 else jnp.concatenate(pieces, axis=1)
        return (sums * scale_ref[:, local_cols:]).astype(BF16)

    def local_weights(projected):
        acc = projected
        sibling = jnp.zeros_like(acc)
        for level in range(local_levels):
            step = 2**level
            swapped = jnp.where(
                (row_lane // step) % 2 == 1,
                pltpu.roll(acc, step, 0),
                pltpu.roll(acc, leaves - step, 0),
            )
            here = (lane >= level * ranks_n) & (lane < (level + 1) * ranks_n)
            sibling = jnp.where(here, swapped, sibling)
            acc = acc + swapped
        return (sibling * scale_ref[:, :local_cols]).astype(BF16)

    def matvec(value, call, out_ref):
        vector = value.astype(BF16)
        ext[call][leaves : 2 * leaves, :] = vector.astype(F32)
        if call == 0:
            pl.semaphore_wait(barrier, n - 1)
        send_halo(call)
        projected = project(vector, call)
        send_far(call)
        weights = local_weights(projected)
        acc = jnp.zeros((leaves, size), F32)
        if call == 0:
            left_copy.wait()
        for c in range(leaves):
            if call == 0 and c % near_width == 0:
                near_copies[c // near_width].wait()
            part = dot_nt(vector, near_v[c, 0]) + dot_nn(
                weights, left_v[0:local_cols, c * size : (c + 1) * size]
            )
            acc = jnp.where(row_size == c, part, acc)
        receive_halo(call)
        for k in range(1, near_n):
            for c in range(leaves):
                position = jnp.clip(index_ref[k, c] - (me - 1) * leaves, 0, 3 * leaves - 1)
                pick[k - 1, c : c + 1, :] = ext[call][pl.ds(position, 1), :]
        picked = [pick[k - 1].astype(BF16) for k in range(1, near_n)]
        for c in range(leaves):
            part = dot_nt(picked[0], near_v[c, 1])
            for k in range(2, near_n):
                part = part + dot_nt(picked[k - 1], near_v[c, k])
            acc = jnp.where(row_size == c, acc + part, acc)
        weights = receive_far(call)
        for c in range(leaves):
            part = dot_nn(weights, left_v[local_cols:cols, c * size : (c + 1) * size])
            acc = jnp.where(row_size == c, acc + part, acc)
        for half in range(2):
            out_ref[pl.ds(half, leaves, stride=2), :] = acc[:, half * LANES : (half + 1) * LANES]
        return acc

    first = matvec(slip, 0, first_ref)
    relaxed = slip + jnp.tanh(first / 3.0)
    matvec(relaxed, 1, second_ref)


def local(slip_rate, near_blocks, near_index, far_left, far_right, far_ranks):
    n = lax.axis_size("leaf")
    leaves, near_n, size, _ = near_blocks.shape
    levels, ranks_n, patches = far_left.shape
    cols = levels * ranks_n
    cross = levels - (leaves.bit_length() - 1)
    chunks = -(-cross * ranks_n // LANES)
    right_parts = 4
    near_parts = 4
    shape = (patches // LANES, LANES)
    vmem = pl.BlockSpec(memory_space=pltpu.VMEM)
    anywhere = pl.BlockSpec(memory_space=pl.ANY)
    first, second = pl.pallas_call(
        functools.partial(kernel, n, levels, ranks_n),
        out_shape=[jax.ShapeDtypeStruct(shape, F32)] * 2,
        in_specs=[
            vmem, anywhere, pl.BlockSpec(memory_space=pltpu.SMEM), anywhere, anywhere, vmem,
        ],
        out_specs=[vmem, vmem],
        scratch_shapes=[
            pltpu.VMEM((leaves, near_n, size, size), BF16),
            pltpu.VMEM((cols, patches), BF16),
            pltpu.VMEM((cols, patches), BF16),
            pltpu.VMEM((3 * leaves, size), F32),
            pltpu.VMEM((3 * leaves, size), F32),
            pltpu.VMEM((near_n - 1, leaves, size), F32),
            pltpu.VMEM((2, chunks, LANES), F32),
            pltpu.VMEM((2, n, LANES), F32),
            pltpu.VMEM((leaves, cols), F32),
            pltpu.SemaphoreType.DMA((near_parts,)),
            pltpu.SemaphoreType.DMA,
            pltpu.SemaphoreType.DMA((right_parts,)),
            pltpu.SemaphoreType.DMA((2, 2)),
            pltpu.SemaphoreType.DMA((2, 2)),
            pltpu.SemaphoreType.DMA((2,)),
            pltpu.SemaphoreType.DMA((2,)),
        ],
        compiler_params=pltpu.CompilerParams(collective_id=0, has_side_effects=True),
    )(
        slip_rate.reshape(shape),
        near_blocks,
        near_index.T,
        far_left.reshape(cols, patches),
        far_right.reshape(cols, patches),
        far_ranks,
    )
    return first.reshape(-1), second.reshape(-1)


def solution(mesh):
    in_specs = (
        P(("models", "leaf")),
        P(("models", "leaf"), None, None, None),
        P(("models", "leaf"), None),
        P(None, None, ("models", "leaf")),
        P(None, None, ("models", "leaf")),
        P(("models", "leaf"), None),
    )
    out_specs = (P(("models", "leaf")), P(("models", "leaf")))
    return jax.shard_map(local, mesh=mesh, in_specs=in_specs, out_specs=out_specs, check_vma=False)
```
